16 devices in a mesh: dz: 2 (over z), dy: 2 (over y), dx: 4 (over x, core).
Axes of the slice: x: 2, y: 2, z: 2, core: 2. Of those that a mesh axis runs over, the one named last changes fastest.
Arguments:
- x_one: bfloat16 [32768, 1024], P(('dz', 'dy', 'dx'))
- g_one: bfloat16 [32768, 1024], P(('dz', 'dy', 'dx'))
- x_two: bfloat16 [32768, 1024], P(('dz', 'dy', 'dx'))
- g_two: bfloat16 [32768, 1024], P(('dz', 'dy', 'dx'))
- w_one: bfloat16 [1024, 4096], replicated
- w_two: bfloat16 [4096, 1024], replicated
- w_three: bfloat16 [1024, 4096], replicated
- w_four: bfloat16 [4096, 1024], replicated
Outputs:
- output 1: float32 [1024, 4096], replicated
- output 2: float32 [4096, 1024], replicated
- output 3: float32 [1024, 4096], replicated
- output 4: float32 [4096, 1024], replicated
- output 5: bfloat16 [32768, 1024], P(('dz', 'dy', 'dx'))
- output 6: bfloat16 [32768, 1024], P(('dz', 'dy', 'dx'))
All inputs are finite; a program needn't handle non-finite values.
Results may differ from the reference program's by a relative error of at most 0.00337683.
Values are sent between devices in bfloat16 or wider.
A program may use at most 1 GiB of HBM per device.

```python
import jax
import jax.numpy as jnp
from jax import lax

D = 1024
FF = 4096
TOKENS_DEV = 2048
DEVICES = 16

GELU_C = 0.7978845608028654
GELU_A = 0.044715


def gelu_value(pre_act):
    pre_f = pre_act.astype(jnp.float32)
    return 0.5 * pre_f * (1.0 + jnp.tanh(GELU_C * (pre_f + GELU_A * pre_f * pre_f * pre_f)))


def gelu_slope(pre_act):
    pre_f = pre_act.astype(jnp.float32)
    tanh_val = jnp.tanh(GELU_C * (pre_f + GELU_A * pre_f * pre_f * pre_f))
    return 0.5 * (1.0 + tanh_val) + 0.5 * pre_f * (1.0 - tanh_val * tanh_val) * GELU_C * (1.0 + 3.0 * GELU_A * pre_f * pre_f)


def local_grads(x_rows, g_rows, w_one, w_two, w_three, w_four):
    pre_one = jnp.dot(x_rows, w_one, preferred_element_type=jnp.float32).astype(jnp.bfloat16)
    act_one = gelu_value(pre_one).astype(jnp.bfloat16)
    act_two = (jnp.dot(act_one, w_two, preferred_element_type=jnp.float32) + x_rows.astype(jnp.float32)).astype(jnp.bfloat16)
    pre_three = jnp.dot(act_two, w_three, preferred_element_type=jnp.float32).astype(jnp.bfloat16)
    act_three = gelu_value(pre_three).astype(jnp.bfloat16)
    grad_four = jnp.dot(act_three.T, g_rows, preferred_element_type=jnp.float32)
    dz_three = (jnp.dot(g_rows, w_four.T, preferred_element_type=jnp.float32) * gelu_slope(pre_three)).astype(jnp.bfloat16)
    grad_three = jnp.dot(act_two.T, dz_three, preferred_element_type=jnp.float32)
    dh_two = (jnp.dot(dz_three, w_three.T, preferred_element_type=jnp.float32) + g_rows.astype(jnp.float32)).astype(jnp.bfloat16)
    grad_two = jnp.dot(act_one.T, dh_two, preferred_element_type=jnp.float32)
    dz_one = (jnp.dot(dh_two, w_two.T, preferred_element_type=jnp.float32) * gelu_slope(pre_one)).astype(jnp.bfloat16)
    grad_one = jnp.dot(x_rows.T, dz_one, preferred_element_type=jnp.float32)
    dx_rows = (jnp.dot(dz_one, w_one.T, preferred_element_type=jnp.float32) + dh_two.astype(jnp.float32)).astype(jnp.bfloat16)
    return (grad_one, grad_two, grad_three, grad_four), dx_rows


def setup_inputs(seed: int = 0) -> dict:
    sub_keys = jax.random.split(jax.random.key(seed), 8)
    total_rows = DEVICES * TOKENS_DEV

    def normal_bf16(sub_key, shape, scale):
        return (jax.random.normal(sub_key, shape, jnp.float32) * scale).astype(jnp.bfloat16)

    return {
        "x_one": normal_bf16(sub_keys[0], (total_rows, D), 1.0),
        "g_one": normal_bf16(sub_keys[1], (total_rows, D), 1.0),
        "x_two": normal_bf16(sub_keys[2], (total_rows, D), 1.0),
        "g_two": normal_bf16(sub_keys[3], (total_rows, D), 1.0),
        "w_one": normal_bf16(sub_keys[4], (D, FF), D ** -0.5),
        "w_two": normal_bf16(sub_keys[5], (FF, D), FF ** -0.5),
        "w_three": normal_bf16(sub_keys[6], (D, FF), D ** -0.5),
        "w_four": normal_bf16(sub_keys[7], (FF, D), FF ** -0.5),
    }


def reference(x_one, g_one, x_two, g_two, w_one, w_two, w_three, w_four):
    block_shape = (DEVICES, TOKENS_DEV, D)
    blocks_in = (x_one.reshape(block_shape), g_one.reshape(block_shape), x_two.reshape(block_shape), g_two.reshape(block_shape))

    def device_step(acc_grads, block_in):
        x_first, g_first, x_second, g_second = block_in
        grads_first, dx_first = local_grads(x_first, g_first, w_one, w_two, w_three, w_four)
        grads_second, dx_second = local_grads(x_second, g_second, w_one, w_two, w_three, w_four)
        new_acc = tuple(acc_part + grad_a + grad_b for acc_part, grad_a, grad_b in zip(acc_grads, grads_first, grads_second))
        return new_acc, (dx_first, dx_second)

    zero_grads = (jnp.zeros((D, FF), jnp.float32), jnp.zeros((FF, D), jnp.float32), jnp.zeros((D, FF), jnp.float32), jnp.zeros((FF, D), jnp.float32))
    sum_grads, dx_blocks = lax.scan(device_step, zero_grads, blocks_in)
    mean_grads = [total_grad / DEVICES for total_grad in sum_grads]
    dx_first_all = dx_blocks[0].reshape(DEVICES * TOKENS_DEV, D)
    dx_second_all = dx_blocks[1].reshape(DEVICES * TOKENS_DEV, D)
    return (mean_grads[0], mean_grads[1], mean_grads[2], mean_grads[3], dx_first_all, dx_second_all)
```

```python
import functools

import jax
import jax.numpy as jnp
from jax import lax
from jax.experimental import pallas as pl
from jax.experimental.pallas import tpu as pltpu
from jax.sharding import PartitionSpec as P


GELU_C = 0.7978845608028654
GELU_A = 0.044715
AXES = ("dz", "dy", "dx")
CHUNK = 256
HALF_STEPS = 8
ROW_BLOCK = 512
VMEM_LIMIT = 67_000_000
A_ROWS = ((0, 40), (40, 40), (80, 48))
B_ROWS = ((0, 48), (48, 40), (88, 40))
SIZES = tuple(a[1] + b[1] for a, b in zip(A_ROWS, B_ROWS))
ORDERS = ((2, 1, 0), (1, 0, 2), (0, 2, 1))


def gelu_value(pre_act):
    pre_f = pre_act.astype(jnp.float32)
    return 0.5 * pre_f * (1.0 + jnp.tanh(GELU_C * (pre_f + GELU_A * pre_f * pre_f * pre_f)))


def mat_tn(left_op, right_op):
    return lax.dot_general(left_op, right_op, (((0,), (0,)), ((), ())), preferred_element_type=jnp.float32)


def mat_nt(left_op, right_op):
    return lax.dot_general(left_op, right_op, (((1,), (1,)), ((), ())), preferred_element_type=jnp.float32)


class Reducer:
    def __init__(self, ua, ub, shard, scratch):
        self.ua, self.ub, self.shard = ua, ub, shard
        (self.acc, self.core_in, self.in_one, self.in_two, self.in_three) = (
            scratch[0:3], scratch[3:6], scratch[6:9], scratch[9:12], scratch[12:15])
        self.own_sem, self.send_sem, self.recv_sem = scratch[15:18]
        dz, dy, dx = lax.axis_index("dz"), lax.axis_index("dy"), lax.axis_index("dx")
        self.core = lax.rem(dx, 2)
        self.bits = (dz, dy, lax.div(dx, 2))
        self.partner = {"dx": dx + 1 - 2 * self.core}
        self.peers = ({"dz": 1 - dz}, {"dy": 1 - dy}, {"dx": lax.rem(dx + 2, 4)})

    def blocks(self, core):
        for part in range(3):
            for source, rows, offset in ((self.ua, A_ROWS[part], 0), (self.ub, B_ROWS[part], A_ROWS[part][1])):
                for index in range(8):
                    zyx = (index // 4, (index // 2) % 2, index % 2)
                    position = tuple(zyx[axis] for axis in ORDERS[part])
                    where = (index * 2) + core
                    yield part, source.at[where, pl.ds(rows[0], rows[1]), :], position, pl.ds(offset, rows[1])

    def begin(self):
        barrier = pltpu.get_barrier_semaphore()
        for device in (self.partner, *self.peers):
            pl.semaphore_signal(barrier, inc=1, device_id=device, device_id_type=pl.DeviceIdType.MESH)
        pl.semaphore_wait(barrier, 4)
        for part, source, (a, b, c), rows in self.blocks(1 - self.core):
            pltpu.make_async_remote_copy(
                src_ref=source, dst_ref=self.core_in[part].at[a, b, c, rows, :],
                send_sem=self.send_sem.at[part], recv_sem=self.recv_sem.at[part],
                device_id=self.partner, device_id_type=pl.DeviceIdType.MESH).start()
        for part, source, (a, b, c), rows in self.blocks(self.core):
            pltpu.make_async_copy(source, self.acc[part].at[a, b, c, rows, :], self.own_sem.at[part]).start()

    def phase_copy(self, phase, part):
        order = ORDERS[part]
        a, b, c = (self.bits[axis] for axis in order)
        acc = self.acc[part]
        if phase == 1:
            source, target = acc.at[1 - a], self.in_one[part]
        elif phase == 2:
            source, target = acc.at[a, 1 - b], self.in_two[part]
        else:
            source, target = acc.at[a, b, 1 - c], self.in_three[part]
        slot = phase * 3 + part
        return pltpu.make_async_remote_copy(
            src_ref=source, dst_ref=target, send_sem=self.send_sem.at[slot], recv_sem=self.recv_sem.at[slot],
            device_id=self.peers[order[phase - 1]], device_id_type=pl.DeviceIdType.MESH)

    def first(self):
        for part in range(3):
            whole = pltpu.make_async_remote_copy(
                src_ref=self.acc[part], dst_ref=self.core_in[part], send_sem=self.send_sem.at[part],
                recv_sem=self.recv_sem.at[part], device_id=self.partner, device_id_type=pl.DeviceIdType.MESH)
            whole.wait_recv()
            whole.wait_send()
            pltpu.make_async_copy(self.acc[part], self.acc[part], self.own_sem.at[part]).wait()
        for part in range(3):
            @pl.loop(0, 4)
            def _(index, part=part):
                a, b = lax.div(index, 2), lax.rem(index, 2)
                self.acc[part][a, b] = self.acc[part][a, b] + self.core_in[part][a, b]

            self.phase_copy(1, part).start()

    def second(self):
        for part in range(3):
            self.phase_copy(1, part).wait()
            a = self.bits[ORDERS[part][0]]
            for b in range(2):
                self.acc[part][a, b] = self.acc[part][a, b] + self.in_one[part][b]
            self.phase_copy(2, part).start()

    def third(self):
        for part in range(3):
            self.phase_copy(2, part).wait()
            a, b = (self.bits[axis] for axis in ORDERS[part][:2])
            self.acc[part][a, b] = self.acc[part][a, b] + self.in_two[part][...]
            self.phase_copy(3, part).start()

    def finish(self):
        for part in range(3):
            self.phase_copy(3, part).wait()
            a, b, c = (self.bits[axis] for axis in ORDERS[part])
            total = (self.acc[part][a, b, c] + self.in_three[part][...]) * (1.0 / 16.0)
            (a0, an), (b0, bn) = A_ROWS[part], B_ROWS[part]
            self.shard[0, 0, a0:a0 + an, :] = total[:an]
            self.shard[0, 1, b0:b0 + bn, :] = total[an:]


def reducer_scratch():
    f32 = jnp.float32
    return [
        *[pltpu.VMEM((2, 2, 2, size, 1024), f32) for size in SIZES],
        *[pltpu.VMEM((2, 2, 2, size, 1024), f32) for size in SIZES],
        *[pltpu.VMEM((2, 2, size, 1024), f32) for size in SIZES],
        *[pltpu.VMEM((2, size, 1024), f32) for size in SIZES],
        *[pltpu.VMEM((size, 1024), f32) for size in SIZES],
        pltpu.SemaphoreType.DMA((3,)),
        pltpu.SemaphoreType.DMA((12,)),
        pltpu.SemaphoreType.DMA((12,)),
    ]


def reduce_kernel(ua, ub, shard, *scratch):
    work = Reducer(ua, ub, shard, scratch)
    work.begin()
    work.first()
    work.second()
    work.third()
    work.finish()


SHARD = jax.ShapeDtypeStruct((1, 2, 128, 1024), jnp.float32)


def reduce_unit(unit, collective_id):
    return pl.pallas_call(
        reduce_kernel,
        out_shape=SHARD,
        in_specs=[pl.BlockSpec(memory_space=pl.ANY)] * 2,
        out_specs=pl.BlockSpec(memory_space=pltpu.VMEM),
        scratch_shapes=reducer_scratch(),
        compiler_params=pltpu.CompilerParams(
            collective_id=collective_id, has_side_effects=True, vmem_limit_bytes=VMEM_LIMIT),
        cost_estimate=pl.CostEstimate(flops=60_000_000_000, bytes_accessed=32 << 20, transcendentals=0),
    )(*unit)


def stage_kernel(rides, schedule, *refs):
    (p_one, p_two, g_one, g_two, at_one, at_two, w_ref), refs = refs[:7], refs[7:]
    if rides:
        (ua_in, ub_in), refs = refs[:2], refs[2:]
    refs = refs[2:] if schedule == "second" else refs
    (dz_one, dz_two, ua, ub), refs = refs[:4], refs[4:]
    if rides:
        shard, refs = refs[0], refs[1:]
    act, refs = refs[0], refs[1:]
    step = pl.program_id(0)
    work = Reducer(ua_in, ub_in, shard, refs) if rides else None

    def ticks(mb):
        if rides:
            for at, action in ((0, work.begin), (3, work.first), (10, work.second), (14, work.third)):
                if at % 2 == mb:
                    pl.when(step == at // 2)(action)

    for mb, (p_ref, g_ref, at_ref, dz_ref) in enumerate(((p_one, g_one, at_one, dz_one), (p_two, g_two, at_two, dz_two))):
        ticks(mb)
        for row in range(0, p_ref.shape[0], ROW_BLOCK):
            rows = pl.ds(row, ROW_BLOCK)
            upstream = mat_nt(g_ref[rows, :], w_ref[...])
            pre = p_ref[rows, :].astype(jnp.float32)
            square = pre * pre
            half = 0.5 + 0.5 * jnp.tanh(pre * (GELU_C + (GELU_C * GELU_A) * square))
            act[rows, :] = (pre * half).astype(jnp.bfloat16)
            slope = half + pre * (half * (1.0 - half)) * (2.0 * GELU_C + (6.0 * GELU_C * GELU_A) * square)
            dz_ref[rows, :] = (upstream * slope).astype(jnp.bfloat16)
        from_act = mat_tn(act[...], g_ref[...]).reshape(ua.shape)
        from_dz = jnp.dot(at_ref[...], dz_ref[...], preferred_element_type=jnp.float32).reshape(ub.shape)
        if mb == 0:
            ua[...] = from_act
            ub[...] = from_dz
        else:
            ua[...] += from_act
            ub[...] += from_dz
    if rides:
        pl.when(step == HALF_STEPS - 1)(work.finish)


def stage(pres, grads, acts_t, weight, second_from=None, ride=None, collective_id=None):
    rows, wide = pres[0].shape
    base = 0 if second_from is None else HALF_STEPS
    resident = pl.Buffered(1)
    column = pl.BlockSpec((rows, CHUNK), lambda c: (0, base + c))
    in_specs = [
        column, column,
        *[pl.BlockSpec((rows, 1024), lambda c: (0, 0), pipeline_mode=resident)] * 2,
        *[pl.BlockSpec((1024, rows), lambda c: (0, 0), pipeline_mode=resident)] * 2,
        pl.BlockSpec((CHUNK, 1024), lambda c: (base + c, 0)),
    ]
    operands = [*pres, *grads, *acts_t, weight]
    any_spec = pl.BlockSpec(memory_space=pl.ANY)
    out_shape = [
        jax.ShapeDtypeStruct((rows, wide), jnp.bfloat16),
        jax.ShapeDtypeStruct((rows, wide), jnp.bfloat16),
        jax.ShapeDtypeStruct((16, 128, 1024), jnp.float32),
        jax.ShapeDtypeStruct((16, 2, 64, 1024), jnp.float32),
    ]
    out_specs = [
        column, column,
        pl.BlockSpec((2, 128, 1024), lambda c: (c, 0, 0)),
        pl.BlockSpec((16, 1, 64, CHUNK), lambda c: (0, c // 4, 0, c % 4)),
    ]
    scratch = [pltpu.VMEM((rows, CHUNK), jnp.bfloat16)]
    params = dict(vmem_limit_bytes=VMEM_LIMIT, dimension_semantics=("arbitrary",))
    if ride is not None:
        operands += list(ride)
        in_specs += [any_spec, any_spec]
        out_shape.append(SHARD)
        out_specs.append(pl.BlockSpec(memory_space=pltpu.VMEM))
        scratch += reducer_scratch()
        params.update(collective_id=collective_id, has_side_effects=True)
    aliases = {}
    if second_from is not None:
        aliases = {len(operands): 0, len(operands) + 1: 1}
        operands += list(second_from)
        in_specs += [any_spec, any_spec]
    flops = 2 * 3 * 2 * rows * 1024 * CHUNK * HALF_STEPS
    out = pl.pallas_call(
        functools.partial(stage_kernel, ride is not None, "second" if second_from is not None else "first"),
        grid=(HALF_STEPS,),
        out_shape=out_shape,
        in_specs=in_specs,
        out_specs=out_specs,
        scratch_shapes=scratch,
        input_output_aliases=aliases,
        compiler_params=pltpu.CompilerParams(**params),
        cost_estimate=pl.CostEstimate(flops=flops, bytes_accessed=80 << 20, transcendentals=0),
    )(*operands)
    unit = (out[2], out[3].reshape(16, 128, 1024))
    return (out[0], out[1]), unit, (out[4] if ride is not None else None)


def assemble_kernel(*refs):
    source, (row_type, col_type) = refs[0], refs[-2:]
    row_type[...] = source[:, 0].reshape(row_type.shape)
    for shard in range(2):
        for side in range(2):
            col_type[shard * 64:(shard + 1) * 64, side * 1024:(side + 1) * 1024] = source[shard, 1, side * 64:(side + 1) * 64, :]


def assemble(gathered, before=None):
    half = 0 if before is None else 1
    operands, in_specs, aliases = [gathered], [pl.BlockSpec((2, 2, 128, 1024), lambda c: (c, 0, 0, 0))], {}
    if before is not None:
        operands += list(before)
        in_specs += [pl.BlockSpec(memory_space=pl.ANY)] * 2
        aliases = {1: 0, 2: 1}
    return pl.pallas_call(
        assemble_kernel,
        grid=(8,),
        out_shape=[jax.ShapeDtypeStruct((4096, 1024), jnp.float32), jax.ShapeDtypeStruct((1024, 4096), jnp.float32)],
        in_specs=in_specs,
        out_specs=[pl.BlockSpec((256, 1024), lambda c: (8 * half + c, 0)), pl.BlockSpec((128, 2048), lambda c: (c, half))],
        input_output_aliases=aliases,
        cost_estimate=pl.CostEstimate(flops=10_000_000, bytes_accessed=32 << 20, transcendentals=0),
    )(*operands)


def solution(mesh):
    row_spec = P(AXES, None)
    rep_spec = P(None, None)

    def forward(x_rows, w_one, w_two, w_three):
        pre_one = jnp.dot(x_rows, w_one, preferred_element_type=jnp.float32).astype(jnp.bfloat16)
        act_one = gelu_value(pre_one).astype(jnp.bfloat16)
        act_two = (jnp.dot(act_one, w_two, preferred_element_type=jnp.float32) + x_rows.astype(jnp.float32)).astype(jnp.bfloat16)
        pre_three = jnp.dot(act_two, w_three, preferred_element_type=jnp.float32).astype(jnp.bfloat16)
        return pre_one, act_two, pre_three

    def through(dz_rows, weight, grad_rows):
        return (mat_nt(dz_rows, weight) + grad_rows.astype(jnp.float32)).astype(jnp.bfloat16)

    def gather(shard):
        return lax.all_gather(shard, AXES, axis=0, tiled=True)

    def whole_step(x_one, g_one, x_two, g_two, w_one, w_two, w_three, w_four):
        pre_a, mid_a, top_a = forward(x_one, w_one, w_two, w_three)
        pre_b, mid_b, top_b = forward(x_two, w_one, w_two, w_three)
        grads = (g_one, g_two)
        mids_t = (mid_a.T, mid_b.T)
        tops = (top_a, top_b)
        dz_three, unit_one, _ = stage(tops, grads, mids_t, w_four)
        dz_three, unit_two, shard_one = stage(tops, grads, mids_t, w_four, dz_three, unit_one, 0)
        whole_one = gather(shard_one)
        dmid = (through(dz_three[0], w_three, g_one), through(dz_three[1], w_three, g_two))
        pres = (pre_a, pre_b)
        xs_t = (x_one.T, x_two.T)
        dz_one, unit_three, shard_two = stage(pres, dmid, xs_t, w_two, None, unit_two, 1)
        whole_two = gather(shard_two)
        dz_one, unit_four, shard_three = stage(pres, dmid, xs_t, w_two, dz_one, unit_three, 2)
        whole_three = gather(shard_three)
        shard_four = reduce_unit(unit_four, 3)
        shard_four, dz_a, dz_b = lax.optimization_barrier((shard_four, dz_one[0], dz_one[1]))
        whole_four = gather(shard_four)
        dx_one, dx_two = through(dz_a, w_one, dmid[0]), through(dz_b, w_one, dmid[1])
        dw_four, dw_three = assemble(whole_two, assemble(whole_one))
        dw_two, dw_one = assemble(whole_four, assemble(whole_three))
        return dw_one, dw_two, dw_three, dw_four, dx_one, dx_two

    return jax.shard_map(
        whole_step,
        mesh=mesh,
        in_specs=(row_spec, row_spec, row_spec, row_spec, rep_spec, rep_spec, rep_spec, rep_spec),
        out_specs=(rep_spec, rep_spec, rep_spec, rep_spec, row_spec, row_spec),
        check_vma=False,
    )
```

```python
import functools

import jax
import jax.numpy as jnp
from jax import lax
from jax.experimental import pallas as pl
from jax.experimental.pallas import tpu as pltpu
from jax.sharding import PartitionSpec as P


GELU_C = 0.7978845608028654
GELU_A = 0.044715
AXES = ("dz", "dy", "dx")
CHUNK = 256
QUARTER = 4
ROW_BLOCK = 512
VMEM_LIMIT = 67_000_000
SHARD_ROWS = 64
XYZ, YZX, ZXY = (2, 1, 0), (1, 0, 2), (0, 2, 1)
PIECES = (
    (0, 0, 40, 0, 1024, XYZ),
    (1, 0, 24, 0, 1024, YZX),
    (1, 24, 40, 0, 1024, ZXY),
    (0, 48, 16, 0, 1024, YZX),
    (0, 40, 8, 0, 512, XYZ),
    (0, 40, 8, 512, 512, YZX),
)
COUNT = len(PIECES)


def gelu_value(pre_act):
    pre_f = pre_act.astype(jnp.float32)
    return 0.5 * pre_f * (1.0 + jnp.tanh(GELU_C * (pre_f + GELU_A * pre_f * pre_f * pre_f)))


def mat_tn(left_op, right_op):
    return lax.dot_general(left_op, right_op, (((0,), (0,)), ((), ())), preferred_element_type=jnp.float32)


def mat_nt(left_op, right_op):
    return lax.dot_general(left_op, right_op, (((1,), (1,)), ((), ())), preferred_element_type=jnp.float32)


MESH = pl.DeviceIdType.MESH


def place():
    dz, dy, dx = lax.axis_index("dz"), lax.axis_index("dy"), lax.axis_index("dx")
    core = lax.rem(dx, 2)
    peers = ({"dz": 1 - dz}, {"dy": 1 - dy}, {"dx": lax.rem(dx + 2, 4)})
    return core, (dz, dy, lax.div(dx, 2)), {"dx": dx + 1 - 2 * core}, peers


def meet():
    _, _, partner, peers = place()
    barrier = pltpu.get_barrier_semaphore()
    for device in (partner, *peers):
        pl.semaphore_signal(barrier, inc=1, device_id=device, device_id_type=MESH)
    pl.semaphore_wait(barrier, 4)


class Early:
    scratch = [
        *[pltpu.VMEM((*lead, piece[2], piece[4]), jnp.float32) for lead in ((2, 2, 2), (2, 2, 2), (2, 2)) for piece in PIECES],
        pltpu.SemaphoreType.DMA((COUNT,)),
        pltpu.SemaphoreType.DMA((2 * COUNT,)),
        pltpu.SemaphoreType.DMA((2 * COUNT,)),
    ]

    def __init__(self, arrays, state, scratch):
        self.arrays, self.state = arrays, state
        self.acc, self.core_in, self.in_one = (scratch[at * COUNT:(at + 1) * COUNT] for at in range(3))
        self.own_sem, self.send_sem, self.recv_sem = scratch[3 * COUNT:]
        self.core, self.bits, self.partner, self.peers = place()

    def blocks(self, core):
        for piece, (array, row, rows, col, cols, order) in enumerate(PIECES):
            for index in range(8):
                zyx = (index // 4, (index // 2) % 2, index % 2)
                source = self.arrays[array].at[(index * 2) + core, pl.ds(row, rows), pl.ds(col, cols)]
                yield piece, source, tuple(zyx[axis] for axis in order)

    def begin(self):
        for piece, source, position in self.blocks(1 - self.core):
            pltpu.make_async_remote_copy(
                src_ref=source, dst_ref=self.core_in[piece].at[position],
                send_sem=self.send_sem.at[piece], recv_sem=self.recv_sem.at[piece],
                device_id=self.partner, device_id_type=MESH).start()
        for piece, source, position in self.blocks(self.core):
            pltpu.make_async_copy(source, self.acc[piece].at[position], self.own_sem.at[piece]).start()

    def axis_copy(self, piece):
        axis = PIECES[piece][-1][0]
        return pltpu.make_async_remote_copy(
            src_ref=self.acc[piece].at[1 - self.bits[axis]], dst_ref=self.in_one[piece],
            send_sem=self.send_sem.at[COUNT + piece], recv_sem=self.recv_sem.at[COUNT + piece],
            device_id=self.peers[axis], device_id_type=MESH)

    def turn(self):
        for piece in range(COUNT):
            whole = pltpu.make_async_remote_copy(
                src_ref=self.acc[piece], dst_ref=self.core_in[piece], send_sem=self.send_sem.at[piece],
                recv_sem=self.recv_sem.at[piece], device_id=self.partner, device_id_type=MESH)
            whole.wait_recv()
            whole.wait_send()
            pltpu.make_async_copy(self.acc[piece], self.acc[piece], self.own_sem.at[piece]).wait()

            @pl.loop(0, 4)
            def _(index, piece=piece):
                a, b = lax.div(index, 2), lax.rem(index, 2)
                self.acc[piece][a, b] = self.acc[piece][a, b] + self.core_in[piece][a, b]

            self.axis_copy(piece).start()

    def finish(self):
        for piece in range(COUNT):
            self.axis_copy(piece).wait()
            a = self.bits[PIECES[piece][-1][0]]
            for b in range(2):
                self.state[piece][b] = self.acc[piece][a, b] + self.in_one[piece][b]


class Late:
    scratch = [
        *[pltpu.VMEM((*lead, piece[2], piece[4]), jnp.float32) for lead in ((2,), (2,), ()) for piece in PIECES],
        pltpu.SemaphoreType.DMA((2 * COUNT,)),
        pltpu.SemaphoreType.DMA((2 * COUNT,)),
    ]

    def __init__(self, state, shard, scratch):
        self.state, self.shard = state, shard
        self.keep, self.in_two, self.in_three = (scratch[at * COUNT:(at + 1) * COUNT] for at in range(3))
        self.send_sem, self.recv_sem = scratch[3 * COUNT:]
        _, self.bits, _, self.peers = place()

    def axis_copy(self, phase, piece):
        axis = PIECES[piece][-1][1 + phase]
        source, target = ((self.state, self.in_two), (self.keep, self.in_three))[phase]
        slot = phase * COUNT + piece
        return pltpu.make_async_remote_copy(
            src_ref=source[piece].at[1 - self.bits[axis]], dst_ref=target[piece],
            send_sem=self.send_sem.at[slot], recv_sem=self.recv_sem.at[slot],
            device_id=self.peers[axis], device_id_type=MESH)

    def begin(self):
        for piece in range(COUNT):
            self.axis_copy(0, piece).start()

    def turn(self):
        for piece in range(COUNT):
            self.axis_copy(0, piece).wait()
            b = self.bits[PIECES[piece][-1][1]]
            self.keep[piece][...] = self.state[piece][b] + self.in_two[piece][...]
            self.axis_copy(1, piece).start()

    def finish(self):
        for piece, (array, row, rows, col, cols, order) in enumerate(PIECES):
            self.axis_copy(1, piece).wait()
            total = (self.keep[piece][self.bits[order[2]]] + self.in_three[piece][...]) * (1.0 / 16.0)
            self.shard[0, array, row:row + rows, col:col + cols] = total


STATE = [jax.ShapeDtypeStruct((2, 2, piece[2], piece[4]), jnp.float32) for piece in PIECES]


def run_at(step, half, work):
    for slot, actions in work.items():
        if slot % 2 == half:
            @pl.when(step == slot // 2)
            def _(actions=actions):
                for action in actions:
                    action()


SHARD = jax.ShapeDtypeStruct((1, 2, SHARD_ROWS, 1024), jnp.float32)
IN_VMEM = pl.BlockSpec(memory_space=pltpu.VMEM)
GROUPS = (1, 1, 1, 1, 1, 1, 2)
ANY = pl.BlockSpec(memory_space=pl.ANY)
RESIDENT = pl.Buffered(1)


def activation_and_slope(pre):
    square = pre * pre
    half = 0.5 + 0.5 * jnp.tanh(pre * (GELU_C + (GELU_C * GELU_A) * square))
    slope = half + pre * (half * (1.0 - half)) * (2.0 * GELU_C + (6.0 * GELU_C * GELU_A) * square)
    return (pre * half).astype(jnp.bfloat16), slope


def stage_kernel(early, late, fused, passed, *refs):
    (in_one, in_two, g_one, g_two, w_ref), refs = refs[:5], refs[5:]
    if fused:
        w_pre, refs = refs[0], refs[1:]
    else:
        (p_one, p_two), refs = refs[:2], refs[2:]
    if early:
        arrays, refs = refs[:2], refs[2:]
    if late:
        state_in, refs = refs[:COUNT], refs[COUNT:]
    if passed:
        refs = refs[2:]
    (dz_one, dz_two, ua, ub), refs = refs[:4], refs[4:]
    if early:
        state_out, refs = refs[:COUNT], refs[COUNT:]
    if late:
        shard, refs = refs[0], refs[1:]
    act, refs = refs[0], refs[1:]
    step = pl.program_id(0)
    work, ends = {}, []
    if early:
        first = Early(arrays, state_out, refs[:len(Early.scratch)])
        work = {0: [meet, first.begin], 2: [first.turn]}
        ends = [first.finish]
    if late:
        second = Late(state_in, shard, refs[len(Early.scratch):])
        work[0].append(second.begin)
        work[4] = [second.turn]
        ends.append(second.finish)
    block = ROW_BLOCK if fused else 2 * ROW_BLOCK
    per_mb = in_one.shape[0] // block

    def block_of(number):
        mb, row = divmod(number, per_mb)
        return mb, pl.ds(row * block, block), (in_one, in_two)[mb], (g_one, g_two)[mb], (dz_one, dz_two)[mb]

    def front(number):
        mb, rows, in_ref, g_ref, _ = block_of(number)
        upstream = mat_nt(g_ref[rows, :], w_ref[...])
        if fused:
            return upstream, jnp.dot(in_ref[rows, :], w_pre[...], preferred_element_type=jnp.float32)
        return upstream, (p_one, p_two)[mb][rows, :]

    def back(number):
        _, rows, in_ref, g_ref, dz_ref = block_of(number)
        from_act = mat_tn(act[rows, :], g_ref[rows, :]).reshape(ua.shape)
        from_dz = mat_tn(dz_ref[rows, :], in_ref[rows, :]).reshape(ub.shape)
        if number == 0:
            ua[...] = from_act
            ub[...] = from_dz
        else:
            ua[...] += from_act
            ub[...] += from_dz

    run_at(step, 0, work)
    ready = front(0)
    for number in range(2 * per_mb):
        upstream, pre = ready
        if number + 1 < 2 * per_mb:
            ready = front(number + 1)
        _, rows, _, _, dz_ref = block_of(number)
        act[rows, :], slope = activation_and_slope(pre.astype(jnp.bfloat16).astype(jnp.float32))
        dz_ref[rows, :] = (upstream * slope).astype(jnp.bfloat16)
        if number:
            back(number - 1)
    back(2 * per_mb - 1)
    for action in ends:
        pl.when(step == QUARTER - 1)(action)


def stage(quarter, ins, grads, weight, w_pre=None, pres=None, passed=None, ride=None):
    rows = ins[0].shape[0]
    hidden = weight.shape[0]
    base = quarter * QUARTER
    column = pl.BlockSpec((rows, CHUNK), lambda c: (0, base + c))
    whole = pl.BlockSpec((rows, 1024), lambda c: (0, 0), pipeline_mode=RESIDENT)
    operands = [*ins, *grads, weight]
    in_specs = [whole] * 4 + [pl.BlockSpec((CHUNK, 1024), lambda c: (base + c, 0))]
    if w_pre is not None:
        operands.append(w_pre)
        in_specs.append(pl.BlockSpec((1024, CHUNK), lambda c: (0, base + c)))
    else:
        operands += list(pres)
        in_specs += [column, column]
    unit_shape = jax.ShapeDtypeStruct((16, SHARD_ROWS, 1024), jnp.float32)
    unit_spec = pl.BlockSpec((CHUNK // SHARD_ROWS, SHARD_ROWS, 1024), lambda c: (c, 0, 0))
    out_shape = [jax.ShapeDtypeStruct((rows, hidden), jnp.bfloat16)] * 2 + [unit_shape] * 2
    out_specs = [column, column, unit_spec, unit_spec]
    scratch = [pltpu.VMEM((rows, CHUNK), jnp.bfloat16)]
    params = dict(vmem_limit_bytes=VMEM_LIMIT, dimension_semantics=("arbitrary",))
    unit, state, collective_id = ride
    if unit is not None:
        operands += list(unit)
        in_specs += [ANY, ANY]
        out_shape += STATE
        out_specs += [IN_VMEM] * COUNT
        scratch += Early.scratch
        params.update(collective_id=collective_id, has_side_effects=True)
    if state is not None:
        operands += list(state)
        in_specs += [IN_VMEM] * COUNT
        out_shape.append(SHARD)
        out_specs.append(IN_VMEM)
        scratch += Late.scratch
    aliases = {}
    if passed is not None:
        aliases = {len(operands): 0, len(operands) + 1: 1}
        operands += list(passed)
        in_specs += [ANY, ANY]
    dots = 4 if w_pre is not None else 3
    out = pl.pallas_call(
        functools.partial(stage_kernel, unit is not None, state is not None, w_pre is not None, passed is not None),
        grid=(QUARTER,),
        out_shape=out_shape,
        in_specs=in_specs,
        out_specs=out_specs,
        scratch_shapes=scratch,
        input_output_aliases=aliases,
        compiler_params=pltpu.CompilerParams(**params),
        cost_estimate=pl.CostEstimate(
            flops=2 * dots * 2 * rows * 1024 * CHUNK * QUARTER, bytes_accessed=48 << 20, transcendentals=0),
    )(*operands)
    half_done = out[4:4 + COUNT] if unit is not None else None
    return (out[0], out[1]), (out[2], out[3]), half_done, (out[-1] if state is not None else None)


DX_ROWS = 512


def last_kernel(early, *refs):
    (dz_ref, add_ref, w_ref), refs = refs[:3], refs[3:]
    if early:
        arrays, refs = refs[:2], refs[2:]
    state_in, dx_ref, refs = refs[:COUNT], refs[COUNT], refs[COUNT + 1:]
    if early:
        state_out, refs = refs[:COUNT], refs[COUNT:]
    shard, refs = refs[0], refs[1:]
    step = pl.program_id(0)
    second = Late(state_in, shard, refs[:len(Late.scratch)])
    work, ends = {0: [meet], 4: []}, []
    if early:
        first = Early(arrays, state_out, refs[len(Late.scratch):])
        work[0].append(first.begin)
        work[4].append(first.turn)
        ends.append(first.finish)
    work[0].append(second.begin)
    work[4].append(second.turn)
    ends.append(second.finish)
    run_at(step, 0, work)
    dx_ref[...] = (mat_nt(dz_ref[...], w_ref[...]) + add_ref[...].astype(jnp.float32)).astype(jnp.bfloat16)
    for action in ends:
        pl.when(step == pl.num_programs(0) - 1)(action)


def last_stage(dz, add, weight, unit, state, collective_id):
    rows, hidden = dz.shape
    wide = pl.BlockSpec((DX_ROWS, hidden), lambda r: (r, 0))
    narrow = pl.BlockSpec((DX_ROWS, 1024), lambda r: (r, 0))
    weight_spec = pl.BlockSpec((1024, hidden), lambda r: (0, 0), pipeline_mode=RESIDENT)
    early = unit is not None
    out = pl.pallas_call(
        functools.partial(last_kernel, early),
        grid=(rows // DX_ROWS,),
        out_shape=[jax.ShapeDtypeStruct((rows, 1024), jnp.bfloat16), *(STATE if early else []), SHARD],
        in_specs=[wide, narrow, weight_spec, *([ANY, ANY] if early else []), *[IN_VMEM] * COUNT],
        out_specs=[narrow, *([IN_VMEM] * COUNT if early else []), IN_VMEM],
        scratch_shapes=[*Late.scratch, *(Early.scratch if early else [])],
        compiler_params=pltpu.CompilerParams(
            collective_id=collective_id, has_side_effects=True, vmem_limit_bytes=VMEM_LIMIT,
            dimension_semantics=("arbitrary",)),
        cost_estimate=pl.CostEstimate(flops=2 * rows * 1024 * hidden, bytes_accessed=32 << 20, transcendentals=0),
    )(dz, add, weight, *(unit if early else ()), *state)
    return out[0], out[1:1 + COUNT] if early else None, out[-1]


FORWARD_CHUNK = 512


def forward_kernel(x_ref, w_one, w_two, pre_ref, mid_ref, acc):
    step = pl.program_id(0)
    count = x_ref.shape[0] // ROW_BLOCK

    @pl.when(step == 0)
    def _():
        acc[...] = x_ref[...].astype(jnp.float32)

    def front(number):
        return jnp.dot(x_ref[pl.ds(number * ROW_BLOCK, ROW_BLOCK), :], w_one[...], preferred_element_type=jnp.float32)

    ready = front(0)
    for number in range(count):
        rows = pl.ds(number * ROW_BLOCK, ROW_BLOCK)
        pre = ready.astype(jnp.bfloat16)
        if number + 1 < count:
            ready = front(number + 1)
        pre_ref[rows, :] = pre
        act = gelu_value(pre).astype(jnp.bfloat16)
        acc[rows, :] += jnp.dot(act, w_two[...], preferred_element_type=jnp.float32)

    @pl.when(step == pl.num_programs(0) - 1)
    def _():
        mid_ref[...] = acc[...].astype(jnp.bfloat16)


def forward(x_rows, w_one, w_two):
    rows, hidden = x_rows.shape[0], w_one.shape[1]
    return pl.pallas_call(
        forward_kernel,
        grid=(hidden // FORWARD_CHUNK,),
        out_shape=[jax.ShapeDtypeStruct((rows, hidden), jnp.bfloat16), jax.ShapeDtypeStruct((rows, 1024), jnp.bfloat16)],
        in_specs=[
            pl.BlockSpec((rows, 1024), lambda c: (0, 0), pipeline_mode=RESIDENT),
            pl.BlockSpec((1024, FORWARD_CHUNK), lambda c: (0, c)),
            pl.BlockSpec((FORWARD_CHUNK, 1024), lambda c: (c, 0)),
        ],
        out_specs=[pl.BlockSpec((rows, FORWARD_CHUNK), lambda c: (0, c)), pl.BlockSpec((rows, 1024), lambda c: (0, 0))],
        scratch_shapes=[pltpu.VMEM((rows, 1024), jnp.float32)],
        compiler_params=pltpu.CompilerParams(vmem_limit_bytes=VMEM_LIMIT, dimension_semantics=("arbitrary",)),
        cost_estimate=pl.CostEstimate(flops=4 * rows * 1024 * hidden, bytes_accessed=40 << 20, transcendentals=0),
    )(x_rows, w_one, w_two)


def assemble_kernel(*refs):
    source, (row_type, col_type) = refs[0], refs[-2:]
    row_type[...] = source[:, 0, 0].reshape(row_type.shape)
    col_type[...] = source[:, 0, 1].reshape(row_type.shape).T


def copy_kernel(one, two, out_one, out_two):
    out_one[...] = one[...]
    out_two[...] = two[...]


def own_buffers(one, two):
    spec = pl.BlockSpec((512, 1024), lambda r: (r, 0))
    return pl.pallas_call(
        copy_kernel,
        grid=(one.shape[0] // 512,),
        out_shape=[jax.ShapeDtypeStruct(one.shape, one.dtype)] * 2,
        in_specs=[spec, spec],
        out_specs=[spec, spec],
        cost_estimate=pl.CostEstimate(flops=10_000_000, bytes_accessed=16 << 20, transcendentals=0),
    )(one, two)


def assemble(quarter, gathered, member, before=None):
    base = quarter * QUARTER
    operands = [gathered]
    in_specs = [pl.BlockSpec((CHUNK // SHARD_ROWS, 1, 2, SHARD_ROWS, 1024), lambda c: (c, member, 0, 0, 0))]
    aliases = {}
    if before is not None:
        operands += list(before)
        in_specs += [ANY, ANY]
        aliases = {1: 0, 2: 1}
    return pl.pallas_call(
        assemble_kernel,
        grid=(QUARTER,),
        out_shape=[jax.ShapeDtypeStruct((4096, 1024), jnp.float32), jax.ShapeDtypeStruct((1024, 4096), jnp.float32)],
        in_specs=in_specs,
        out_specs=[pl.BlockSpec((CHUNK, 1024), lambda c: (base + c, 0)), pl.BlockSpec((1024, CHUNK), lambda c: (0, base + c))],
        input_output_aliases=aliases,
        cost_estimate=pl.CostEstimate(flops=10_000_000, bytes_accessed=16 << 20, transcendentals=0),
    )(*operands)


def solution(mesh):
    row_spec = P(AXES, None)
    rep_spec = P(None, None)

    def through(dz_rows, weight, grad_rows):
        return (mat_nt(dz_rows, weight) + grad_rows.astype(jnp.float32)).astype(jnp.bfloat16)

    def gather(shards):
        whole = lax.all_gather(jnp.stack(shards, axis=1), AXES, axis=0, tiled=True)
        return [(whole, member) for member in range(len(shards))]

    def whole_step(x_one, g_one, x_two, g_two, w_one, w_two, w_three, w_four):
        pres_and_mids = (forward(x_one, w_one, w_two), forward(x_two, w_one, w_two))
        pres = tuple(pair[0] for pair in pres_and_mids)
        mids = tuple(pair[1] for pair in pres_and_mids)
        wholes, waiting = [], []
        unit = state = None
        rides = groups = 0

        def collect(shard):
            nonlocal groups
            waiting.append(shard)
            if len(waiting) == GROUPS[groups]:
                wholes.extend(gather(waiting))
                waiting.clear()
                groups += 1

        def quarter_of(quarter, *operands, **named):
            nonlocal unit, state, rides
            rides += unit is not None
            ride = (unit, state, rides)
            dzs, unit, state, shard = stage(quarter, *operands, ride=ride, **named)
            if shard is not None:
                collect(shard)
            return dzs

        dz_three = None
        for quarter in range(4):
            dz_three = quarter_of(quarter, mids, (g_one, g_two), w_four, w_pre=w_three, passed=dz_three)
        dmid = (through(dz_three[0], w_three, g_one), through(dz_three[1], w_three, g_two))
        dz_one = None
        for quarter in range(4):
            dz_one = quarter_of(quarter, (x_one, x_two), dmid, w_two, pres=pres, passed=dz_one)
        dx_one, state, shard = last_stage(dz_one[0], dmid[0], w_one, unit, state, 8)
        collect(shard)
        dx_two, _, shard = last_stage(dz_one[1], dmid[1], w_one, None, state, 9)
        collect(shard)
        dx_one, dx_two = own_buffers(dx_one, dx_two)
        upper = lower = None
        for quarter in range(4):
            upper = assemble(quarter, *wholes[quarter], upper)
        for quarter in range(4):
            if quarter == 3:
                lower, upper, dx_one, dx_two = lax.optimization_barrier((lower, upper, dx_one, dx_two))
            lower = assemble(quarter, *wholes[4 + quarter], lower)
        return lower[1], lower[0], upper[1], upper[0], dx_one, dx_two

    return jax.shard_map(
        whole_step,
        mesh=mesh,
        in_specs=(row_spec, row_spec, row_spec, row_spec, rep_spec, rep_spec, rep_spec, rep_spec),
        out_specs=(rep_spec, rep_spec, rep_spec, rep_spec, row_spec, row_spec),
        check_vma=False,
    )
```

```python
import functools

import jax
import jax.numpy as jnp
from jax import lax
from jax.experimental import pallas as pl
from jax.experimental.pallas import tpu as pltpu
from jax.sharding import PartitionSpec as P


GELU_C = 0.7978845608028654
GELU_A = 0.044715
AXES = ("dz", "dy", "dx")
CHUNK = 256
QUARTER = 4
ROW_BLOCK = 512
VMEM_LIMIT = 67_000_000
SHARD_ROWS = 64
XYZ, YZX, ZXY = (2, 1, 0), (1, 0, 2), (0, 2, 1)
PIECES = (
    (0, 0, 40, 0, 1024, XYZ),
    (1, 0, 24, 0, 1024, YZX),
    (1, 24, 40, 0, 1024, ZXY),
    (0, 48, 16, 0, 1024, YZX),
    (0, 40, 8, 0, 512, XYZ),
    (0, 40, 8, 512, 512, YZX),
)
COUNT = len(PIECES)


def gelu_value(pre_act):
    pre_f = pre_act.astype(jnp.float32)
    return 0.5 * pre_f * (1.0 + jnp.tanh(GELU_C * (pre_f + GELU_A * pre_f * pre_f * pre_f)))


def mat_tn(left_op, right_op):
    return lax.dot_general(left_op, right_op, (((0,), (0,)), ((), ())), preferred_element_type=jnp.float32)


def mat_nt(left_op, right_op):
    return lax.dot_general(left_op, right_op, (((1,), (1,)), ((), ())), preferred_element_type=jnp.float32)


MESH = pl.DeviceIdType.MESH


def place():
    dz, dy, dx = lax.axis_index("dz"), lax.axis_index("dy"), lax.axis_index("dx")
    core = lax.rem(dx, 2)
    peers = ({"dz": 1 - dz}, {"dy": 1 - dy}, {"dx": lax.rem(dx + 2, 4)})
    return core, (dz, dy, lax.div(dx, 2)), {"dx": dx + 1 - 2 * core}, peers


def meet():
    _, _, partner, peers = place()
    barrier = pltpu.get_barrier_semaphore()
    for device in (partner, *peers):
        pl.semaphore_signal(barrier, inc=1, device_id=device, device_id_type=MESH)
    pl.semaphore_wait(barrier, 4)


class Early:
    scratch = [
        *[pltpu.VMEM((*lead, piece[2], piece[4]), jnp.float32) for lead in ((2, 2, 2), (2, 2, 2), (2, 2)) for piece in PIECES],
        pltpu.SemaphoreType.DMA((COUNT,)),
        pltpu.SemaphoreType.DMA((2 * COUNT,)),
        pltpu.SemaphoreType.DMA((2 * COUNT,)),
    ]

    def __init__(self, arrays, state, scratch):
        self.arrays, self.state = arrays, state
        self.acc, self.core_in, self.in_one = (scratch[at * COUNT:(at + 1) * COUNT] for at in range(3))
        self.own_sem, self.send_sem, self.recv_sem = scratch[3 * COUNT:]
        self.core, self.bits, self.partner, self.peers = place()

    def blocks(self, core):
        for piece, (array, row, rows, col, cols, order) in enumerate(PIECES):
            for index in range(8):
                zyx = (index // 4, (index // 2) % 2, index % 2)
                source = self.arrays[array].at[(index * 2) + core, pl.ds(row, rows), pl.ds(col, cols)]
                yield piece, source, tuple(zyx[axis] for axis in order)

    def begin(self):
        for piece, source, position in self.blocks(1 - self.core):
            pltpu.make_async_remote_copy(
                src_ref=source, dst_ref=self.core_in[piece].at[position],
                send_sem=self.send_sem.at[piece], recv_sem=self.recv_sem.at[piece],
                device_id=self.partner, device_id_type=MESH).start()
        for piece, source, position in self.blocks(self.core):
            pltpu.make_async_copy(source, self.acc[piece].at[position], self.own_sem.at[piece]).start()

    def axis_copy(self, piece):
        axis = PIECES[piece][-1][0]
        return pltpu.make_async_remote_copy(
            src_ref=self.acc[piece].at[1 - self.bits[axis]], dst_ref=self.in_one[piece],
            send_sem=self.send_sem.at[COUNT + piece], recv_sem=self.recv_sem.at[COUNT + piece],
            device_id=self.peers[axis], device_id_type=MESH)

    def turn(self):
        for piece in range(COUNT):
            whole = pltpu.make_async_remote_copy(
                src_ref=self.acc[piece], dst_ref=self.core_in[piece], send_sem=self.send_sem.at[piece],
                recv_sem=self.recv_sem.at[piece], device_id=self.partner, device_id_type=MESH)
            whole.wait_recv()
            whole.wait_send()
            pltpu.make_async_copy(self.acc[piece], self.acc[piece], self.own_sem.at[piece]).wait()

            @pl.loop(0, 4)
            def _(index, piece=piece):
                a, b = lax.div(index, 2), lax.rem(index, 2)
                self.acc[piece][a, b] = self.acc[piece][a, b] + self.core_in[piece][a, b]

            self.axis_copy(piece).start()

    def finish(self):
        for piece in range(COUNT):
            self.axis_copy(piece).wait()
            a = self.bits[PIECES[piece][-1][0]]
            for b in range(2):
                self.state[piece][b] = self.acc[piece][a, b] + self.in_one[piece][b]


class Late:
    scratch = [
        *[pltpu.VMEM((*lead, piece[2], piece[4]), jnp.float32) for lead in ((2,), (2,), ()) for piece in PIECES],
        pltpu.SemaphoreType.DMA((2 * COUNT,)),
        pltpu.SemaphoreType.DMA((2 * COUNT,)),
    ]

    def __init__(self, state, shard, scratch):
        self.state, self.shard = state, shard
        self.keep, self.in_two, self.in_three = (scratch[at * COUNT:(at + 1) * COUNT] for at in range(3))
        self.send_sem, self.recv_sem = scratch[3 * COUNT:]
        _, self.bits, _, self.peers = place()

    def axis_copy(self, phase, piece):
        axis = PIECES[piece][-1][1 + phase]
        source, target = ((self.state, self.in_two), (self.keep, self.in_three))[phase]
        slot = phase * COUNT + piece
        return pltpu.make_async_remote_copy(
            src_ref=source[piece].at[1 - self.bits[axis]], dst_ref=target[piece],
            send_sem=self.send_sem.at[slot], recv_sem=self.recv_sem.at[slot],
            device_id=self.peers[axis], device_id_type=MESH)

    def begin(self):
        for piece in range(COUNT):
            self.axis_copy(0, piece).start()

    def turn(self):
        for piece in range(COUNT):
            self.axis_copy(0, piece).wait()
            b = self.bits[PIECES[piece][-1][1]]
            self.keep[piece][...] = self.state[piece][b] + self.in_two[piece][...]
            self.axis_copy(1, piece).start()

    def finish(self):
        for piece, (array, row, rows, col, cols, order) in enumerate(PIECES):
            self.axis_copy(1, piece).wait()
            total = (self.keep[piece][self.bits[order[2]]] + self.in_three[piece][...]) * (1.0 / 16.0)
            self.shard[0, array, row:row + rows, col:col + cols] = total


STATE = [jax.ShapeDtypeStruct((2, 2, piece[2], piece[4]), jnp.float32) for piece in PIECES]


def run_at(step, half, work):
    for slot, actions in work.items():
        if slot % 2 == half:
            @pl.when(step == slot // 2)
            def _(actions=actions):
                for action in actions:
                    action()


SHARD = jax.ShapeDtypeStruct((1, 2, SHARD_ROWS, 1024), jnp.float32)
IN_VMEM = pl.BlockSpec(memory_space=pltpu.VMEM)
GROUPS = (1, 1, 1, 1, 1, 1, 2)
ANY = pl.BlockSpec(memory_space=pl.ANY)
RESIDENT = pl.Buffered(1)


def activation_and_slope(pre):
    square = pre * pre
    half = 0.5 + 0.5 * jnp.tanh(pre * (GELU_C + (GELU_C * GELU_A) * square))
    slope = half + pre * (half * (1.0 - half)) * (2.0 * GELU_C + (6.0 * GELU_C * GELU_A) * square)
    return (pre * half).astype(jnp.bfloat16), slope


def stage_kernel(early, late, fused, passed, *refs):
    (in_one, in_two, g_one, g_two, w_ref), refs = refs[:5], refs[5:]
    if fused:
        w_pre, refs = refs[0], refs[1:]
    else:
        (p_one, p_two), refs = refs[:2], refs[2:]
    if early:
        arrays, refs = refs[:2], refs[2:]
    if late:
        state_in, refs = refs[:COUNT], refs[COUNT:]
    if passed:
        refs = refs[2:]
    (dz_one, dz_two, ua, ub), refs = refs[:4], refs[4:]
    if early:
        state_out, refs = refs[:COUNT], refs[COUNT:]
    if late:
        shard, refs = refs[0], refs[1:]
    act, refs = refs[0], refs[1:]
    step = pl.program_id(0)
    work, ends = {}, []
    if early:
        first = Early(arrays, state_out, refs[:len(Early.scratch)])
        work = {0: [meet, first.begin], 2: [first.turn]}
        ends = [first.finish]
    if late:
        second = Late(state_in, shard, refs[len(Early.scratch):])
        work[0].append(second.begin)
        work[4] = [second.turn]
        ends.append(second.finish)
    block = ROW_BLOCK if fused else 2 * ROW_BLOCK
    per_mb = in_one.shape[0] // block

    def block_of(number):
        mb, row = divmod(number, per_mb)
        return mb, pl.ds(row * block, block), (in_one, in_two)[mb], (g_one, g_two)[mb], (dz_one, dz_two)[mb]

    def front(number):
        mb, rows, in_ref, g_ref, _ = block_of(number)
        upstream = mat_nt(g_ref[rows, :], w_ref[...])
        if fused:
            return upstream, jnp.dot(in_ref[rows, :], w_pre[...], preferred_element_type=jnp.float32)
        return upstream, (p_one, p_two)[mb][rows, :]

    def back(number):
        _, rows, in_ref, g_ref, dz_ref = block_of(number)
        from_act = mat_tn(act[rows, :], g_ref[rows, :]).reshape(ua.shape)
        from_dz = mat_tn(dz_ref[rows, :], in_ref[rows, :]).reshape(ub.shape)
        if number == 0:
            ua[...] = from_act
            ub[...] = from_dz
        else:
            ua[...] += from_act
            ub[...] += from_dz

    run_at(step, 0, work)
    ready = front(0)
    for number in range(2 * per_mb):
        upstream, pre = ready
        if number + 1 < 2 * per_mb:
            ready = front(number + 1)
        _, rows, _, _, dz_ref = block_of(number)
        act[rows, :], slope = activation_and_slope(pre.astype(jnp.bfloat16).astype(jnp.float32))
        dz_ref[rows, :] = (upstream * slope).astype(jnp.bfloat16)
        if number:
            back(number - 1)
    back(2 * per_mb - 1)
    for action in ends:
        pl.when(step == QUARTER - 1)(action)


def stage(unit, state, quarter, ins, grads, weight, collective_id, w_pre=None, pres=None, passed=None):
    rows = ins[0].shape[0]
    hidden = weight.shape[0]
    base = quarter * QUARTER
    column = pl.BlockSpec((rows, CHUNK), lambda c: (0, base + c))
    whole = pl.BlockSpec((rows, 1024), lambda c: (0, 0), pipeline_mode=RESIDENT)
    operands = [*ins, *grads, weight]
    in_specs = [whole] * 4 + [pl.BlockSpec((CHUNK, 1024), lambda c: (base + c, 0))]
    if w_pre is not None:
        operands.append(w_pre)
        in_specs.append(pl.BlockSpec((1024, CHUNK), lambda c: (0, base + c)))
    else:
        operands += list(pres)
        in_specs += [column, column]
    unit_shape = jax.ShapeDtypeStruct((16, SHARD_ROWS, 1024), jnp.float32)
    unit_spec = pl.BlockSpec((CHUNK // SHARD_ROWS, SHARD_ROWS, 1024), lambda c: (c, 0, 0))
    out_shape = [jax.ShapeDtypeStruct((rows, hidden), jnp.bfloat16)] * 2 + [unit_shape] * 2
    out_specs = [column, column, unit_spec, unit_spec]
    scratch = [pltpu.VMEM((rows, CHUNK), jnp.bfloat16)]
    params = dict(vmem_limit_bytes=VMEM_LIMIT, dimension_semantics=("arbitrary",))
    if unit is not None:
        operands += list(unit)
        in_specs += [ANY, ANY]
        out_shape += STATE
        out_specs += [IN_VMEM] * COUNT
        scratch += Early.scratch
        params.update(collective_id=collective_id, has_side_effects=True)
    if state is not None:
        operands += list(state)
        in_specs += [IN_VMEM] * COUNT
        out_shape.append(SHARD)
        out_specs.append(IN_VMEM)
        scratch += Late.scratch
    aliases = {}
    if passed is not None:
        aliases = {len(operands): 0, len(operands) + 1: 1}
        operands += list(passed)
        in_specs += [ANY, ANY]
    dots = 4 if w_pre is not None else 3
    out = pl.pallas_call(
        functools.partial(stage_kernel, unit is not None, state is not None, w_pre is not None, passed is not None),
        grid=(QUARTER,),
        out_shape=out_shape,
        in_specs=in_specs,
        out_specs=out_specs,
        scratch_shapes=scratch,
        input_output_aliases=aliases,
        compiler_params=pltpu.CompilerParams(**params),
        cost_estimate=pl.CostEstimate(
            flops=2 * dots * 2 * rows * 1024 * CHUNK * QUARTER, bytes_accessed=48 << 20, transcendentals=0),
    )(*operands)
    half_done = out[4:4 + COUNT] if unit is not None else None
    return (out[0], out[1]), (out[2], out[3]), half_done, (out[-1] if state is not None else None)


DX_ROWS = 512


def last_kernel(early, *refs):
    (dz_ref, add_ref, w_ref), refs = refs[:3], refs[3:]
    if early:
        arrays, refs = refs[:2], refs[2:]
    state_in, dx_ref, refs = refs[:COUNT], refs[COUNT], refs[COUNT + 1:]
    if early:
        state_out, refs = refs[:COUNT], refs[COUNT:]
    shard, refs = refs[0], refs[1:]
    step = pl.program_id(0)
    second = Late(state_in, shard, refs[:len(Late.scratch)])
    work, ends = {0: [meet], 4: []}, []
    if early:
        first = Early(arrays, state_out, refs[len(Late.scratch):])
        work[0].append(first.begin)
        work[4].append(first.turn)
        ends.append(first.finish)
    work[0].append(second.begin)
    work[4].append(second.turn)
    ends.append(second.finish)
    run_at(step, 0, work)
    dx_ref[...] = (mat_nt(dz_ref[...], w_ref[...]) + add_ref[...].astype(jnp.float32)).astype(jnp.bfloat16)
    for action in ends:
        pl.when(step == pl.num_programs(0) - 1)(action)


def last_stage(unit, state, dz, add, weight, collective_id):
    rows, hidden = dz.shape
    wide = pl.BlockSpec((DX_ROWS, hidden), lambda r: (r, 0))
    narrow = pl.BlockSpec((DX_ROWS, 1024), lambda r: (r, 0))
    weight_spec = pl.BlockSpec((1024, hidden), lambda r: (0, 0), pipeline_mode=RESIDENT)
    early = unit is not None
    out = pl.pallas_call(
        functools.partial(last_kernel, early),
        grid=(rows // DX_ROWS,),
        out_shape=[jax.ShapeDtypeStruct((rows, 1024), jnp.bfloat16), *(STATE if early else []), SHARD],
        in_specs=[wide, narrow, weight_spec, *([ANY, ANY] if early else []), *[IN_VMEM] * COUNT],
        out_specs=[narrow, *([IN_VMEM] * COUNT if early else []), IN_VMEM],
        scratch_shapes=[*Late.scratch, *(Early.scratch if early else [])],
        compiler_params=pltpu.CompilerParams(
            collective_id=collective_id, has_side_effects=True, vmem_limit_bytes=VMEM_LIMIT,
            dimension_semantics=("arbitrary",)),
        cost_estimate=pl.CostEstimate(flops=2 * rows * 1024 * hidden, bytes_accessed=32 << 20, transcendentals=0),
    )(dz, add, weight, *(unit if early else ()), *state)
    return out[0], out[1:1 + COUNT] if early else None, out[-1]


FORWARD_CHUNK = 512


def forward_kernel(x_ref, w_one, w_two, pre_ref, mid_ref, acc):
    step = pl.program_id(0)
    count = x_ref.shape[0] // ROW_BLOCK

    @pl.when(step == 0)
    def _():
        acc[...] = x_ref[...].astype(jnp.float32)

    def front(number):
        return jnp.dot(x_ref[pl.ds(number * ROW_BLOCK, ROW_BLOCK), :], w_one[...], preferred_element_type=jnp.float32)

    ready = front(0)
    for number in range(count):
        rows = pl.ds(number * ROW_BLOCK, ROW_BLOCK)
        pre = ready.astype(jnp.bfloat16)
        if number + 1 < count:
            ready = front(number + 1)
        pre_ref[rows, :] = pre
        act = gelu_value(pre).astype(jnp.bfloat16)
        acc[rows, :] += jnp.dot(act, w_two[...], preferred_element_type=jnp.float32)

    @pl.when(step == pl.num_programs(0) - 1)
    def _():
        mid_ref[...] = acc[...].astype(jnp.bfloat16)


def forward(x_rows, w_one, w_two):
    rows, hidden = x_rows.shape[0], w_one.shape[1]
    return pl.pallas_call(
        forward_kernel,
        grid=(hidden // FORWARD_CHUNK,),
        out_shape=[jax.ShapeDtypeStruct((rows, hidden), jnp.bfloat16), jax.ShapeDtypeStruct((rows, 1024), jnp.bfloat16)],
        in_specs=[
            pl.BlockSpec((rows, 1024), lambda c: (0, 0), pipeline_mode=RESIDENT),
            pl.BlockSpec((1024, FORWARD_CHUNK), lambda c: (0, c)),
            pl.BlockSpec((FORWARD_CHUNK, 1024), lambda c: (c, 0)),
        ],
        out_specs=[pl.BlockSpec((rows, FORWARD_CHUNK), lambda c: (0, c)), pl.BlockSpec((rows, 1024), lambda c: (0, 0))],
        scratch_shapes=[pltpu.VMEM((rows, 1024), jnp.float32)],
        compiler_params=pltpu.CompilerParams(vmem_limit_bytes=VMEM_LIMIT, dimension_semantics=("arbitrary",)),
        cost_estimate=pl.CostEstimate(flops=4 * rows * 1024 * hidden, bytes_accessed=40 << 20, transcendentals=0),
    )(x_rows, w_one, w_two)


def assemble_kernel(*refs):
    source, (row_type, col_type) = refs[0], refs[-2:]
    row_type[...] = source[:, 0, 0].reshape(row_type.shape)
    col_type[...] = source[:, 0, 1].reshape(row_type.shape).T


def copy_kernel(one, two, out_one, out_two):
    out_one[...] = one[...]
    out_two[...] = two[...]


def own_buffers(one, two):
    spec = pl.BlockSpec((512, 1024), lambda r: (r, 0))
    return pl.pallas_call(
        copy_kernel,
        grid=(one.shape[0] // 512,),
        out_shape=[jax.ShapeDtypeStruct(one.shape, one.dtype)] * 2,
        in_specs=[spec, spec],
        out_specs=[spec, spec],
        cost_estimate=pl.CostEstimate(flops=10_000_000, bytes_accessed=16 << 20, transcendentals=0),
    )(one, two)


def assemble(quarter, gathered, member, before=None):
    base = quarter * QUARTER
    operands = [gathered]
    in_specs = [pl.BlockSpec((CHUNK // SHARD_ROWS, 1, 2, SHARD_ROWS, 1024), lambda c: (c, member, 0, 0, 0))]
    aliases = {}
    if before is not None:
        operands += list(before)
        in_specs += [ANY, ANY]
        aliases = {1: 0, 2: 1}
    return pl.pallas_call(
        assemble_kernel,
        grid=(QUARTER,),
        out_shape=[jax.ShapeDtypeStruct((4096, 1024), jnp.float32), jax.ShapeDtypeStruct((1024, 4096), jnp.float32)],
        in_specs=in_specs,
        out_specs=[pl.BlockSpec((CHUNK, 1024), lambda c: (base + c, 0)), pl.BlockSpec((1024, CHUNK), lambda c: (0, base + c))],
        input_output_aliases=aliases,
        cost_estimate=pl.CostEstimate(flops=10_000_000, bytes_accessed=16 << 20, transcendentals=0),
    )(*operands)


def solution(mesh):
    row_spec = P(AXES, None)
    rep_spec = P(None, None)

    def gather(shards):
        whole = lax.all_gather(jnp.stack(shards, axis=1), AXES, axis=0, tiled=True)
        return [(whole, member) for member in range(len(shards))]

    def whole_step(x_one, g_one, x_two, g_two, w_one, w_two, w_three, w_four):
        pres_and_mids = (forward(x_one, w_one, w_two), forward(x_two, w_one, w_two))
        pres = tuple(pair[0] for pair in pres_and_mids)
        mids = tuple(pair[1] for pair in pres_and_mids)
        wholes, waiting = [], []
        unit = state = None
        rides = groups = 0

        def collect(shard):
            nonlocal groups
            waiting.append(shard)
            if len(waiting) == GROUPS[groups]:
                wholes.extend(gather(waiting))
                waiting.clear()
                groups += 1

        def numbered(kernel, *operands, **named):
            nonlocal rides
            results = kernel(*operands, rides, **named)
            rides += 1
            if results[-1] is not None:
                collect(results[-1])
            return results[:-1]

        dz_three = None
        for quarter in range(4):
            dz_three, unit, state = numbered(
                stage, unit, state, quarter, mids, (g_one, g_two), w_four, w_pre=w_three, passed=dz_three)
        dmid_one, state = numbered(last_stage, unit, state, dz_three[0], g_one, w_three)
        dmid_two, _ = numbered(last_stage, None, state, dz_three[1], g_two, w_three)
        dmid = (dmid_one, dmid_two)
        dz_one = unit = state = None
        for quarter in range(4):
            dz_one, unit, state = numbered(
                stage, unit, state, quarter, (x_one, x_two), dmid, w_two, pres=pres, passed=dz_one)
        dx_one, state = numbered(last_stage, unit, state, dz_one[0], dmid[0], w_one)
        dx_two, _ = numbered(last_stage, None, state, dz_one[1], dmid[1], w_one)
        dx_one, dx_two = own_buffers(dx_one, dx_two)
        upper = lower = None
        for quarter in range(4):
            upper = assemble(quarter, *wholes[quarter], upper)
        for quarter in range(4):
            if quarter == 3:
                lower, upper, dx_one, dx_two = lax.optimization_barrier((lower, upper, dx_one, dx_two))
            lower = assemble(quarter, *wholes[4 + quarter], lower)
        return lower[1], lower[0], upper[1], upper[0], dx_one, dx_two

    return jax.shard_map(
        whole_step,
        mesh=mesh,
        in_specs=(row_spec, row_spec, row_spec, row_spec, rep_spec, rep_spec, rep_spec, rep_spec),
        out_specs=(rep_spec, rep_spec, rep_spec, rep_spec, row_spec, row_spec),
        check_vma=False,
    )
```
